16 devices in a mesh: dp: 2 (over y, z), sp: 8 (over x, core).
Axes of the slice: x: 4, y: 2, z: 1, core: 2. Of those that a mesh axis runs over, the one named last changes fastest.
The devices are a block of a 4x4x8 slice.
Arguments:
- resid: float32 [32, 512, 2560], P('dp', 'sp'), parts along dimension 0
- pre_norm: float32 [2, 2560], replicated
- w_in: bfloat16 [2, 2560, 10576], replicated
- conv_w: float32 [2, 5376, 4], replicated
- conv_b: float32 [2, 5376], replicated
- dt_bias: float32 [2, 80], replicated
- a_log: float32 [2, 80], replicated
- d_skip: float32 [2, 80], replicated
- gate_norm: float32 [2, 1, 5120], replicated
- w_out: bfloat16 [2, 5120, 2560], replicated
Outputs:
- output 1: float32 [32, 512, 2560], P('dp', 'sp'), parts along dimension 0
- output 2: float32 [32, 2, 80, 64, 128], P('dp', None, 'sp'), parts along dimension 0
- output 3: bfloat16 [32, 2, 5376, 3], P('dp'), parts along dimension 0
There are 2 independent parts. The reference program is written for one: setup_inputs(seed, part) draws one part's arguments, and reference() takes and returns one part's arrays. A program takes and returns all parts, laid end to end along the dimension named above; an argument that names none is the same for every part.
All inputs are finite; a program needn't handle non-finite values.
Results may differ from the reference program's by a relative error of at most 0.017196.
Values are sent between devices in bfloat16 or wider.
A program may use at most 768 MiB of HBM per device.

```python
import jax
import jax.numpy as jnp
from jax import lax

D_MODEL = 2560
D_INNER = 5120
NUM_HEADS = 80
HEAD_DIM = 64
NUM_GROUPS = 1
D_STATE = 128
BATCH = 16
SEQ_LEN = 512
LAYERS = 2
CONV_WIDTH = 4
CHUNK = 256

CONV_DIM = D_INNER + 2 * NUM_GROUPS * D_STATE
IN_DIM = D_INNER + CONV_DIM + NUM_HEADS
PER_GROUP = NUM_HEADS // NUM_GROUPS
GROUP_WIDTH = D_INNER // NUM_GROUPS
EPSILON = 1e-5


def setup_inputs(seed: int = 0, part: int = 0) -> dict:
    key = jax.random.key(seed)
    keys = jax.random.split(key, 9)
    part_key = jax.random.fold_in(key, part)
    resid = jax.random.normal(part_key, (BATCH, SEQ_LEN, D_MODEL), jnp.float32)
    pre_norm = jax.random.uniform(keys[0], (LAYERS, D_MODEL), jnp.float32, 0.5, 1.5)
    w_in = (jax.random.normal(keys[1], (LAYERS, D_MODEL, IN_DIM), jnp.float32) * D_MODEL ** -0.5).astype(jnp.bfloat16)
    bc_weight = 1.5 * (SEQ_LEN * D_STATE) ** -0.25
    column_scale = jnp.concatenate([jnp.full((D_INNER,), 0.5, jnp.float32), jnp.full((2 * NUM_GROUPS * D_STATE,), bc_weight, jnp.float32)])
    conv_w = jax.random.normal(keys[2], (LAYERS, CONV_DIM, CONV_WIDTH), jnp.float32) * column_scale[:, None]
    conv_b = jax.random.normal(keys[3], (LAYERS, CONV_DIM), jnp.float32) * 0.5 * column_scale
    dt_bias = jax.random.uniform(keys[4], (LAYERS, NUM_HEADS), jnp.float32, -1.0, 1.0)
    a_log = jnp.log(jax.random.uniform(keys[5], (LAYERS, NUM_HEADS), jnp.float32, 0.5, 2.0) / SEQ_LEN)
    d_skip = jax.random.uniform(keys[6], (LAYERS, NUM_HEADS), jnp.float32, 0.5, 1.5)
    gate_norm = jax.random.uniform(keys[7], (LAYERS, NUM_GROUPS, GROUP_WIDTH), jnp.float32, 0.5, 1.5)
    w_out = (jax.random.normal(keys[8], (LAYERS, D_INNER, D_MODEL), jnp.float32) * D_INNER ** -0.5).astype(jnp.bfloat16)
    return {'resid': resid, 'pre_norm': pre_norm, 'w_in': w_in, 'conv_w': conv_w, 'conv_b': conv_b, 'dt_bias': dt_bias, 'a_log': a_log, 'd_skip': d_skip, 'gate_norm': gate_norm, 'w_out': w_out}


def rms_norm(values, gain_vec):
    mean_sq = jnp.mean(values * values, axis=-1, keepdims=True)
    return values * lax.rsqrt(mean_sq + EPSILON) * gain_vec


def ssd_sequence(x_sequence, dt_sequence, b_sequence, c_sequence, a_neg):
    n_chunks = SEQ_LEN // CHUNK
    x_scaled = (x_sequence * dt_sequence[:, :, None]).reshape(n_chunks, CHUNK, NUM_GROUPS, PER_GROUP, HEAD_DIM)
    log_decay = (dt_sequence * a_neg).reshape(n_chunks, CHUNK, NUM_GROUPS, PER_GROUP)
    b_chunks = b_sequence.reshape(n_chunks, CHUNK, NUM_GROUPS, D_STATE)
    c_chunks = c_sequence.reshape(n_chunks, CHUNK, NUM_GROUPS, D_STATE)
    causal = jnp.arange(CHUNK)[:, None] >= jnp.arange(CHUNK)[None, :]

    def chunk_step(state, chunk_data):
        x_chunk, log_chunk, b_chunk, c_chunk = chunk_data
        cum_log = jnp.cumsum(log_chunk, axis=0)
        cum_heads = jnp.transpose(cum_log, (1, 2, 0))
        log_diff = cum_heads[:, :, :, None] - cum_heads[:, :, None, :]
        decay_mat = jnp.exp(jnp.where(causal, log_diff, -jnp.inf))
        scores = jnp.einsum('tgn,sgn->gts', c_chunk, b_chunk)
        mix_mat = decay_mat * scores[:, None]
        y_intra = jnp.einsum('ghts,sghp->tghp', mix_mat, x_chunk)
        y_inter = jnp.einsum('tgn,ghpn->tghp', c_chunk, state) * jnp.exp(cum_log)[:, :, :, None]
        to_end = jnp.exp(cum_log[-1] - cum_log)
        new_state = state * jnp.exp(cum_log[-1])[:, :, None, None] + jnp.einsum('sghp,sgn->ghpn', x_chunk * to_end[:, :, :, None], b_chunk)
        return new_state, y_intra + y_inter

    state_zero = jnp.zeros((NUM_GROUPS, PER_GROUP, HEAD_DIM, D_STATE), jnp.float32)
    final, y_chunks = lax.scan(chunk_step, state_zero, (x_scaled, log_decay, b_chunks, c_chunks))
    return y_chunks.reshape(SEQ_LEN, NUM_HEADS, HEAD_DIM), final.reshape(NUM_HEADS, HEAD_DIM, D_STATE)


def mamba_layer(resid, pre_w, w_in_l, conv_w_l, conv_b_l, dt_b, a_log_l, d_l, gate_w, w_out_l):
    normed = rms_norm(resid, pre_w).astype(jnp.bfloat16)
    projected = jnp.dot(normed.reshape(-1, D_MODEL), w_in_l, preferred_element_type=jnp.float32).astype(jnp.bfloat16).reshape(BATCH, SEQ_LEN, IN_DIM)
    gate_z = projected[:, :, :D_INNER]
    xbc = projected[:, :, D_INNER:D_INNER + CONV_DIM]
    dt_raw = projected[:, :, D_INNER + CONV_DIM:]
    padded = jnp.pad(xbc, ((0, 0), (CONV_WIDTH - 1, 0), (0, 0))).astype(jnp.float32)
    conv_out = conv_b_l + sum(padded[:, tap_index:tap_index + SEQ_LEN] * conv_w_l[:, tap_index] for tap_index in range(CONV_WIDTH))
    activated = jax.nn.silu(conv_out).astype(jnp.bfloat16)
    x_act = activated[:, :, :D_INNER].reshape(BATCH, SEQ_LEN, NUM_HEADS, HEAD_DIM)
    b_act = activated[:, :, D_INNER:D_INNER + NUM_GROUPS * D_STATE].reshape(BATCH, SEQ_LEN, NUM_GROUPS, D_STATE)
    c_act = activated[:, :, D_INNER + NUM_GROUPS * D_STATE:].reshape(BATCH, SEQ_LEN, NUM_GROUPS, D_STATE)
    delta = jax.nn.softplus(dt_raw.astype(jnp.float32) + dt_b).astype(jnp.bfloat16)
    a_neg = -jnp.exp(a_log_l)

    def one_sequence(seq_parts):
        x_part, dt_part, b_part, c_part = seq_parts
        return ssd_sequence(x_part.astype(jnp.float32), dt_part.astype(jnp.float32), b_part.astype(jnp.float32), c_part.astype(jnp.float32), a_neg)

    y_ssm, final = lax.map(one_sequence, (x_act, delta, b_act, c_act))
    y_full = (y_ssm + d_l[:, None] * x_act.astype(jnp.float32)).astype(jnp.bfloat16)
    gated = y_full.astype(jnp.float32).reshape(BATCH, SEQ_LEN, D_INNER) * jax.nn.silu(gate_z.astype(jnp.float32))
    grouped = gated.reshape(BATCH, SEQ_LEN, NUM_GROUPS, GROUP_WIDTH)
    normed_y = (grouped * lax.rsqrt(jnp.mean(grouped * grouped, axis=-1, keepdims=True) + EPSILON) * gate_w).astype(jnp.bfloat16)
    out_proj = jnp.dot(normed_y.reshape(-1, D_INNER), w_out_l, preferred_element_type=jnp.float32).reshape(BATCH, SEQ_LEN, D_MODEL)
    tail_rows = jnp.swapaxes(xbc[:, SEQ_LEN - (CONV_WIDTH - 1):], 1, 2)
    return resid + out_proj, final, tail_rows


def reference(resid, pre_norm, w_in, conv_w, conv_b, dt_bias, a_log, d_skip, gate_norm, w_out):
    def layer_step(carry, layer_weights):
        pre_w, w_in_l, conv_w_l, conv_b_l, dt_b, a_log_l, d_l, gate_w, w_out_l = layer_weights
        new_resid, final, tail_rows = mamba_layer(carry, pre_w, w_in_l, conv_w_l, conv_b_l, dt_b, a_log_l, d_l, gate_w, w_out_l)
        return new_resid, (final, tail_rows)

    out_resid, (finals, tails) = lax.scan(layer_step, resid, (pre_norm, w_in, conv_w, conv_b, dt_bias, a_log, d_skip, gate_norm, w_out))
    return out_resid, jnp.swapaxes(finals, 0, 1), jnp.swapaxes(tails, 0, 1)
```

```python
import functools

import jax
import jax.numpy as jnp
from jax import lax
from jax.experimental import pallas as pl
from jax.experimental.pallas import tpu as pltpu
from jax.sharding import PartitionSpec as P

CONV_WIDTH = 4
EPSILON = 1e-5
LANES = 128
CHUNKS = 4


def conv_kernel(n_prompts, seg_len, width, n_heads, x_ref, bc_ref, dtr_ref, xh_ref, bch_ref, wx_ref, wbc_ref, bx_ref, bbc_ref, dtb_ref, sel_ref, out_ref, bc_keep, dt_keep):
    dest = pl.program_id(0)
    taps = CONV_WIDTH - 1
    blocks = width // LANES

    def conv(cur, halo, w, bias):
        cur = cur.astype(jnp.float32)
        halo = halo.astype(jnp.float32)
        acc = bias + cur * w[taps:taps + 1]
        for back in range(1, CONV_WIDTH):
            shifted = jnp.concatenate([halo[taps - back:], cur[:seg_len - back]], axis=0)
            acc = acc + shifted * w[taps - back:taps - back + 1]
        return (acc * jax.nn.sigmoid(acc)).astype(jnp.bfloat16)

    @pl.when(dest == 0)
    def _():
        raw = dtr_ref[...].astype(jnp.float32)
        column = lax.broadcasted_iota(jnp.int32, raw.shape, 1)
        delta = jax.nn.softplus(raw + dtb_ref[...])
        delta = jnp.where(column < n_heads, delta, 0.0).astype(jnp.bfloat16)
        rows = lax.dot_general(sel_ref[...], delta, (((1,), (1,)), ((), ())), preferred_element_type=jnp.float32)
        rows = rows.astype(jnp.bfloat16)
        for d in range(dt_keep.shape[0]):
            for part in range(dt_keep.shape[1] // 16):
                dt_keep[d, part * 16:(part + 1) * 16] = rows[d * 16:(d + 1) * 16, part * LANES:(part + 1) * LANES]

    @pl.when(dest < 2)
    def _():
        for p in range(n_prompts):
            bc_keep[dest, p] = conv(bc_ref[p * seg_len:(p + 1) * seg_len], bch_ref[p], wbc_ref[...], bbc_ref[...])

    parity = lax.rem(dest, 2)
    per_prompt = (blocks + 1) * seg_len
    for p in range(n_prompts):
        for j in range(blocks):
            cols = slice(j * LANES, (j + 1) * LANES)
            out_ref[0, p * per_prompt + j * seg_len:p * per_prompt + (j + 1) * seg_len] = conv(
                x_ref[p * seg_len:(p + 1) * seg_len, cols], xh_ref[p, :, cols], wx_ref[:, cols], bx_ref[:, cols])
        out_ref[0, p * per_prompt + blocks * seg_len:(p + 1) * per_prompt] = bc_keep[parity, p]
    out_ref[0, n_prompts * per_prompt:] = dt_keep[dest]


def conv_call(u, halo, conv_w, conv_b, dt_b, select, sizes):
    n_prompts, seg_len, d_inner, conv_dim, n_heads, n_dest = sizes
    width = d_inner // n_dest
    blocks = width // LANES
    dt_rows = n_prompts * seg_len // LANES * 16
    rows = n_prompts * (blocks + 1) * seg_len + dt_rows
    tokens = n_prompts * seg_len
    x0 = d_inner // width
    bc0 = 2 * d_inner // LANES
    dt0 = (d_inner + conv_dim) // LANES
    taps = CONV_WIDTH - 1
    body = functools.partial(conv_kernel, n_prompts, seg_len, width, n_heads)
    parity = lambda d: lax.rem(d, 2)
    return pl.pallas_call(
        body,
        grid=(n_dest,),
        in_specs=[
            pl.BlockSpec((tokens, width), lambda d: (0, x0 + d)),
            pl.BlockSpec((tokens, LANES), lambda d: (0, bc0 + parity(d))),
            pl.BlockSpec((tokens, LANES), lambda d: (0, dt0)),
            pl.BlockSpec((n_prompts, taps, width), lambda d: (0, 0, d)),
            pl.BlockSpec((n_prompts, taps, LANES), lambda d: (0, 0, d_inner // LANES + parity(d))),
            pl.BlockSpec((CONV_WIDTH, width), lambda d: (0, d)),
            pl.BlockSpec((CONV_WIDTH, LANES), lambda d: (0, d_inner // LANES + parity(d))),
            pl.BlockSpec((1, width), lambda d: (0, d)),
            pl.BlockSpec((1, LANES), lambda d: (0, d_inner // LANES + parity(d))),
            pl.BlockSpec((1, LANES), lambda d: (0, 0)),
            pl.BlockSpec((n_dest * 16, LANES), lambda d: (0, 0)),
        ],
        out_specs=pl.BlockSpec((1, rows, LANES), lambda d: (d, 0, 0)),
        out_shape=jax.ShapeDtypeStruct((n_dest, rows, LANES), jnp.bfloat16),
        scratch_shapes=[
            pltpu.VMEM((2, n_prompts, seg_len, LANES), jnp.bfloat16),
            pltpu.VMEM((n_dest, dt_rows, LANES), jnp.bfloat16),
        ],
        compiler_params=pltpu.CompilerParams(vmem_limit_bytes=16 * 1024 * 1024),
        cost_estimate=pl.CostEstimate(flops=tokens * d_inner * 60, bytes_accessed=4 * tokens * d_inner, transcendentals=tokens * d_inner),
        name='conv_pack',
    )(u, u, u, halo, halo, conv_w, conv_w, conv_b, conv_b, dt_b, select)


def scan_kernel(seg_count, seg_len, blocks, n_local, head_dim, par_ref, x_ref, other_ref, dt_ref, a_ref, d_ref, *rest):
    y_ref, fin_ref, state = rest[-3:]
    per_chunk = LANES // seg_len
    pairs = LANES // head_dim
    tokens = LANES
    even = par_ref[0] == 0
    row = lax.broadcasted_iota(jnp.int32, (tokens, tokens), 0)
    col = lax.broadcasted_iota(jnp.int32, (tokens, tokens), 1)
    causal = row >= col
    first = col < head_dim
    lane = lax.broadcasted_iota(jnp.int32, (16, tokens), 1)
    a_neg = a_ref[...]
    for half in range(LANES // seg_len):
        per_prompt = (blocks + 1) * seg_len
        base = half * per_prompt
        state[...] = jnp.zeros_like(state)
        for chunk in range(seg_count // per_chunk):
            segs = range(chunk * per_chunk, (chunk + 1) * per_chunk)
            tok = lambda ref, lo: jnp.concatenate([ref[s, lo:lo + seg_len] for s in segs], axis=0)
            mine = tok(x_ref, base + blocks * seg_len)
            other = tok(other_ref, half * seg_len)
            b_mat = jnp.where(even, mine, other)
            c_mat = jnp.where(even, other, mine)
            dt = jnp.concatenate([dt_ref[s, :16, half * seg_len:(half + 1) * seg_len] for s in segs], axis=1).astype(jnp.float32)
            cum = dt * a_neg
            step = 1
            while step < tokens:
                cum = cum + jnp.where(lane >= step, pltpu.roll(cum, step, 1), 0.0)
                step *= 2
            last = cum[:, tokens - 1:]
            weight = jnp.exp(last - cum) * dt
            cum_c = cum.T
            dt_c = dt.T
            exp_c = jnp.exp(cum_c)
            weight_c = weight.T
            last_e = jnp.exp(last)
            scores = lax.dot_general(c_mat, b_mat, (((1,), (1,)), ((), ())), preferred_element_type=jnp.float32)
            scores = jnp.where(causal, scores, 0.0)
            for j in range(blocks):
                heads = [j * pairs + k for k in range(pairs)]
                pick = lambda arr: jnp.where(first, arr[:, heads[0]:heads[0] + 1], arr[:, heads[1]:heads[1] + 1])
                mixes = []
                for h in heads:
                    diff = jnp.where(causal, cum_c[:, h:h + 1] - cum[h:h + 1, :], -jnp.inf)
                    mixes.append((jnp.exp(diff) * scores).astype(jnp.bfloat16))
                x2 = tok(x_ref, base + j * seg_len).astype(jnp.float32)
                xs = (x2 * pick(dt_c)).astype(jnp.bfloat16)
                zero = jnp.zeros_like(xs)
                stacked = jnp.concatenate([jnp.where(first, xs, zero), jnp.where(first, zero, xs)], axis=0)
                y_intra = jnp.dot(jnp.concatenate(mixes, axis=1), stacked, preferred_element_type=jnp.float32)
                s_old = state[j * LANES:(j + 1) * LANES]
                y_inter = lax.dot_general(c_mat, s_old.astype(jnp.bfloat16), (((1,), (1,)), ((), ())), preferred_element_type=jnp.float32)
                y = y_intra + y_inter * pick(exp_c) + d_ref[:, j * LANES:(j + 1) * LANES] * x2
                y = y.astype(jnp.bfloat16)
                for k, s in enumerate(segs):
                    y_ref[s, (half * blocks + j) * seg_len:(half * blocks + j + 1) * seg_len] = y[k * seg_len:(k + 1) * seg_len]
                xw = (x2 * pick(weight_c)).astype(jnp.bfloat16)
                gain = lax.dot_general(xw, b_mat, (((0,), (0,)), ((), ())), preferred_element_type=jnp.float32)
                decay = jnp.concatenate([jnp.broadcast_to(last_e[h:h + 1], (head_dim, 1)) for h in heads], axis=0)
                state[j * LANES:(j + 1) * LANES] = s_old * decay + gain
        for h in range(n_local):
            fin_ref[half, 0, h] = state[h * head_dim:(h + 1) * head_dim]


def scan_call(parity, packed, other, a_neg, d_wide, finals, place, sizes):
    n_prompts, seg_len, seg_count, n_local, head_dim, d_state, batch, layers = sizes
    blocks = n_local * head_dim // LANES
    group = LANES // seg_len
    per_prompt = (blocks + 1) * seg_len
    dt_first = n_prompts * per_prompt // 16
    layer_index, first_prompt = place
    steps = n_prompts // group
    body = functools.partial(scan_kernel, seg_count, seg_len, blocks, n_local, head_dim)
    in_specs = [
        pl.BlockSpec(memory_space=pltpu.SMEM),
        pl.BlockSpec((seg_count, group * per_prompt, LANES), lambda g: (0, g, 0)),
        pl.BlockSpec((seg_count, group * seg_len, LANES), lambda g: (0, g, 0)),
        pl.BlockSpec((seg_count, 16, LANES), lambda g: (0, dt_first + g, 0)),
        pl.BlockSpec((16, LANES), lambda g: (0, 0)),
        pl.BlockSpec((1, n_local * head_dim), lambda g: (0, 0)),
    ]
    operands = [parity, packed, other, packed, a_neg, d_wide]
    aliases = {}
    if finals is not None:
        in_specs.append(pl.BlockSpec(memory_space=pl.ANY))
        operands.append(finals)
        aliases = {6: 1}
    tokens = n_prompts * seg_len * seg_count
    return pl.pallas_call(
        body,
        grid=(steps,),
        in_specs=in_specs,
        out_specs=[
            pl.BlockSpec((seg_count, group * blocks * seg_len, LANES), lambda g: (0, g, 0)),
            pl.BlockSpec((group, 1, n_local, head_dim, d_state), lambda g: (first_prompt // group + g, layer_index, 0, 0, 0)),
        ],
        out_shape=[
            jax.ShapeDtypeStruct((seg_count, n_prompts * blocks * seg_len, LANES), jnp.bfloat16),
            jax.ShapeDtypeStruct((batch, layers, n_local, head_dim, d_state), jnp.float32),
        ],
        scratch_shapes=[pltpu.VMEM((n_local * head_dim, d_state), jnp.float32)],
        input_output_aliases=aliases,
        compiler_params=pltpu.CompilerParams(vmem_limit_bytes=24 * 1024 * 1024),
        cost_estimate=pl.CostEstimate(flops=tokens * n_local * 16000, bytes_accessed=tokens * n_local * head_dim * 6, transcendentals=tokens * n_local * LANES),
        name='scan',
    )(*operands)


def gate_kernel(n_src, blocks, seg_len, y_ref, z_ref, w_ref, out_ref, keep):
    total = jnp.zeros((seg_len, LANES), jnp.float32)
    for d in range(n_src):
        for j in range(blocks):
            cols = slice((d * blocks + j) * LANES, (d * blocks + j + 1) * LANES)
            z = z_ref[:, cols].astype(jnp.float32)
            g = y_ref[d, j * seg_len:(j + 1) * seg_len].astype(jnp.float32) * (z * jax.nn.sigmoid(z))
            keep[:, cols] = g
            total = total + g * g
    width = n_src * blocks * LANES
    scale = lax.rsqrt(jnp.sum(total, axis=1, keepdims=True) / width + EPSILON)
    for i in range(n_src * blocks):
        cols = slice(i * LANES, (i + 1) * LANES)
        out_ref[:, cols] = (keep[:, cols] * scale * w_ref[:, cols]).astype(jnp.bfloat16)


def gate_call(y, u, gate_w, n_prompts, seg_len, d_inner):
    n_src = y.shape[0]
    blocks = d_inner // n_src // LANES
    tokens = n_prompts * seg_len
    return pl.pallas_call(
        functools.partial(gate_kernel, n_src, blocks, seg_len),
        grid=(n_prompts,),
        in_specs=[
            pl.BlockSpec((n_src, blocks * seg_len, LANES), lambda p: (0, p, 0)),
            pl.BlockSpec((seg_len, d_inner), lambda p: (p, 0)),
            pl.BlockSpec((1, d_inner), lambda p: (0, 0)),
        ],
        out_specs=pl.BlockSpec((seg_len, d_inner), lambda p: (p, 0)),
        out_shape=jax.ShapeDtypeStruct((tokens, d_inner), jnp.bfloat16),
        scratch_shapes=[pltpu.VMEM((seg_len, d_inner), jnp.float32)],
        compiler_params=pltpu.CompilerParams(vmem_limit_bytes=16 * 1024 * 1024),
        cost_estimate=pl.CostEstimate(flops=tokens * d_inner * 40, bytes_accessed=6 * tokens * d_inner, transcendentals=tokens * d_inner),
        name='gate',
    )(y, u, gate_w)


def solution(mesh):
    seg_count = mesh.shape['sp']

    def forward(resid, pre_norm, w_in, conv_w, conv_b, dt_bias, a_log, d_skip, gate_norm, w_out):
        batch, seg_len, d_model = resid.shape
        layers, n_heads = dt_bias.shape
        conv_dim = conv_b.shape[1]
        d_inner = gate_norm.shape[1] * gate_norm.shape[2]
        d_state = (conv_dim - d_inner) // 2
        head_dim = d_inner // n_heads
        n_local = n_heads // seg_count
        n_prompts = batch // CHUNKS
        blocks = n_local * head_dim // LANES
        per_prompt = (blocks + 1) * seg_len
        taps = CONV_WIDTH - 1
        seg_index = lax.axis_index('sp')
        parity = lax.rem(seg_index, 2).astype(jnp.int32).reshape(1)
        forward_pairs = [(source, source + 1) for source in range(seg_count - 1)]
        core_pairs = [(source, source ^ 1) for source in range(seg_count)]

        slot = jnp.arange(seg_count * 16)
        wanted = jnp.where(slot % 16 < n_local, slot // 16 * n_local + slot % 16, -1)
        select = (wanted[:, None] == jnp.arange(LANES)[None, :]).astype(jnp.bfloat16)
        pad_heads = lambda values: jnp.pad(values, ((0, 0), (0, LANES - n_heads)))
        dt_bias_wide = pad_heads(dt_bias)
        conv_wt = jnp.swapaxes(conv_w, 1, 2)

        finals = None
        tails = []
        streams = [resid[c * n_prompts:(c + 1) * n_prompts].reshape(n_prompts * seg_len, d_model) for c in range(CHUNKS)]
        for l in range(layers):
            mine = lax.dynamic_slice_in_dim(a_log[l], seg_index * n_local, n_local)
            a_neg = jnp.broadcast_to(jnp.pad(-jnp.exp(mine), (0, 16 - n_local))[:, None], (16, LANES))
            d_wide = jnp.repeat(lax.dynamic_slice_in_dim(d_skip[l], seg_index * n_local, n_local), head_dim)[None]
            layer_tails = []
            for c in range(CHUNKS):
                r = streams[c]
                with jax.named_scope(f'in{l}_{c}'):
                    h = (r * lax.rsqrt(jnp.mean(r * r, axis=-1, keepdims=True) + EPSILON) * pre_norm[l]).astype(jnp.bfloat16)
                    u = jnp.dot(h, w_in[l], preferred_element_type=jnp.float32).astype(jnp.bfloat16)
                    tail = u.reshape(n_prompts, seg_len, -1)[:, seg_len - taps:, d_inner:d_inner + conv_dim]
                    halo = lax.ppermute(tail, 'sp', forward_pairs)
                    layer_tails.append(tail)
                    packed = conv_call(u, halo, conv_wt[l], conv_b[l:l + 1], dt_bias_wide[l:l + 1], select, (n_prompts, seg_len, d_inner, conv_dim, n_heads, seg_count))
                with jax.named_scope(f'go{l}_{c}'):
                    packed = lax.all_to_all(packed, 'sp', 0, 0, tiled=True)
                with jax.named_scope(f'scan{l}_{c}'):
                    bc = packed[:, :n_prompts * per_prompt].reshape(seg_count, n_prompts, blocks + 1, seg_len, LANES)[:, :, blocks]
                    other = lax.ppermute(bc.reshape(seg_count, n_prompts * seg_len, LANES), 'sp', core_pairs)
                    y, finals = scan_call(parity, packed, other, a_neg, d_wide, finals, (l, c * n_prompts), (n_prompts, seg_len, seg_count, n_local, head_dim, d_state, batch, layers))
                with jax.named_scope(f'back{l}_{c}'):
                    y = lax.all_to_all(y, 'sp', 0, 0, tiled=True)
                with jax.named_scope(f'out{l}_{c}'):
                    g = gate_call(y, u, gate_norm[l], n_prompts, seg_len, d_inner)
                    streams[c] = r + jnp.dot(g, w_out[l], preferred_element_type=jnp.float32)
            tails.append(jnp.concatenate(layer_tails, axis=0))
        tail_rows = jnp.stack(tails, axis=2)
        tail_rows = jnp.where(seg_index == seg_count - 1, tail_rows, jnp.zeros((), jnp.bfloat16))
        conv_state = lax.psum(tail_rows, 'sp')
        out = jnp.concatenate(streams, axis=0).reshape(batch, seg_len, d_model)
        return out, finals, jnp.transpose(conv_state, (0, 2, 3, 1))

    return jax.shard_map(forward, mesh=mesh, in_specs=(P('dp', 'sp', None), P(), P(), P(), P(), P(), P(), P(), P(), P()), out_specs=(P('dp', 'sp', None), P('dp', None, 'sp', None, None), P('dp', None, None, None)), check_vma=False)
```

```python
import functools

import jax
import jax.numpy as jnp
from jax import lax
from jax.experimental import pallas as pl
from jax.experimental.pallas import tpu as pltpu
from jax.sharding import PartitionSpec as P


CONV_WIDTH = 4
EPSILON = 1e-5
LANES = 128
SIZES = (8, 8)


def conv_kernel(n_prompts, seg_len, width, n_heads, x_ref, bc_ref, dtr_ref, xh_ref, bch_ref, wx_ref, wbc_ref, bx_ref, bbc_ref, dtb_ref, sel_ref, out_ref, bc_keep, dt_keep):
    dest = pl.program_id(0)
    taps = CONV_WIDTH - 1
    blocks = width // LANES

    def conv(cur, halo, w, bias):
        cur = cur.astype(jnp.float32)
        halo = halo.astype(jnp.float32)
        acc = bias + cur * w[taps:taps + 1]
        for back in range(1, CONV_WIDTH):
            shifted = jnp.concatenate([halo[taps - back:], cur[:seg_len - back]], axis=0)
            acc = acc + shifted * w[taps - back:taps - back + 1]
        return (acc * jax.nn.sigmoid(acc)).astype(jnp.bfloat16)

    @pl.when(dest == 0)
    def _():
        raw = dtr_ref[...].astype(jnp.float32)
        column = lax.broadcasted_iota(jnp.int32, raw.shape, 1)
        delta = jax.nn.softplus(raw + dtb_ref[...])
        delta = jnp.where(column < n_heads, delta, 0.0).astype(jnp.bfloat16)
        rows = lax.dot_general(sel_ref[...], delta, (((1,), (1,)), ((), ())), preferred_element_type=jnp.float32)
        rows = rows.astype(jnp.bfloat16)
        for d in range(dt_keep.shape[0]):
            for part in range(dt_keep.shape[1] // 16):
                dt_keep[d, part * 16:(part + 1) * 16] = rows[d * 16:(d + 1) * 16, part * LANES:(part + 1) * LANES]

    @pl.when(dest < 2)
    def _():
        for p in range(n_prompts):
            bc_keep[dest, p] = conv(bc_ref[p * seg_len:(p + 1) * seg_len], bch_ref[:, p], wbc_ref[...], bbc_ref[...])

    parity = lax.rem(dest, 2)
    per_prompt = blocks * seg_len
    bc_start = n_prompts * per_prompt
    for p in range(n_prompts):
        for j in range(blocks):
            cols = slice(j * LANES, (j + 1) * LANES)
            out_ref[0, p * per_prompt + j * seg_len:p * per_prompt + (j + 1) * seg_len] = conv(
                x_ref[p * seg_len:(p + 1) * seg_len, cols], xh_ref[:, p, cols], wx_ref[:, cols], bx_ref[:, cols])
        out_ref[0, bc_start + p * seg_len:bc_start + (p + 1) * seg_len] = bc_keep[parity, p]
    out_ref[0, bc_start + n_prompts * seg_len:] = dt_keep[dest]


def tail_kernel(n_prompts, seg_len, u_ref, out_ref):
    taps = CONV_WIDTH - 1
    for k in range(taps):
        rows = [u_ref[(p + 1) * seg_len - 16:(p + 1) * seg_len].astype(jnp.float32)[16 - taps + k:17 - taps + k] for p in range(n_prompts)]
        out_ref[k] = jnp.concatenate(rows, axis=0).astype(jnp.bfloat16)


def tail_call(u, n_prompts, seg_len, conv_dim):
    taps = CONV_WIDTH - 1
    width = 6 * LANES
    return pl.pallas_call(
        functools.partial(tail_kernel, n_prompts, seg_len),
        grid=(conv_dim // width,),
        in_specs=[pl.BlockSpec((n_prompts * seg_len, width), lambda i: (0, i))],
        out_specs=pl.BlockSpec((taps, n_prompts, width), lambda i: (0, 0, i)),
        out_shape=jax.ShapeDtypeStruct((taps, n_prompts, conv_dim), jnp.bfloat16),
        cost_estimate=pl.CostEstimate(flops=n_prompts * conv_dim * 100, bytes_accessed=2 * n_prompts * seg_len * conv_dim, transcendentals=0),
        name='tail',
    )(u)


def conv_call(u, halo, conv_w, conv_b, dt_b, select, sizes):
    n_prompts, seg_len, d_inner, conv_dim, n_heads, n_dest = sizes
    width = d_inner // n_dest
    blocks = width // LANES
    dt_rows = n_prompts * seg_len // LANES * 16
    rows = n_prompts * (blocks + 1) * seg_len + dt_rows
    tokens = n_prompts * seg_len
    bc0 = d_inner // LANES
    dt0 = conv_dim // LANES
    taps = CONV_WIDTH - 1
    body = functools.partial(conv_kernel, n_prompts, seg_len, width, n_heads)
    parity = lambda d: lax.rem(d, 2)
    return pl.pallas_call(
        body,
        grid=(n_dest,),
        in_specs=[
            pl.BlockSpec((tokens, width), lambda d: (0, d)),
            pl.BlockSpec((tokens, LANES), lambda d: (0, bc0 + parity(d))),
            pl.BlockSpec((tokens, LANES), lambda d: (0, dt0)),
            pl.BlockSpec((taps, n_prompts, width), lambda d: (0, 0, d)),
            pl.BlockSpec((taps, n_prompts, LANES), lambda d: (0, 0, d_inner // LANES + parity(d))),
            pl.BlockSpec((CONV_WIDTH, width), lambda d: (0, d)),
            pl.BlockSpec((CONV_WIDTH, LANES), lambda d: (0, d_inner // LANES + parity(d))),
            pl.BlockSpec((1, width), lambda d: (0, d)),
            pl.BlockSpec((1, LANES), lambda d: (0, d_inner // LANES + parity(d))),
            pl.BlockSpec((1, LANES), lambda d: (0, 0)),
            pl.BlockSpec((n_dest * 16, LANES), lambda d: (0, 0)),
        ],
        out_specs=pl.BlockSpec((1, rows, LANES), lambda d: (d, 0, 0)),
        out_shape=jax.ShapeDtypeStruct((n_dest, rows, LANES), jnp.bfloat16),
        scratch_shapes=[
            pltpu.VMEM((2, n_prompts, seg_len, LANES), jnp.bfloat16),
            pltpu.VMEM((n_dest, dt_rows, LANES), jnp.bfloat16),
        ],
        cost_estimate=pl.CostEstimate(flops=tokens * d_inner * 60, bytes_accessed=4 * tokens * d_inner, transcendentals=tokens * d_inner),
        name='conv_pack',
    )(u, u, u, halo, halo, conv_w, conv_w, conv_b, conv_b, dt_b, select)


def scan_kernel(seg_count, seg_len, blocks, n_local, head_dim, par_ref, x_ref, mine_ref, other_ref, dt_ref, a_ref, d_ref, *rest):
    y_ref, fin_ref, state = rest[-3:]
    tokens = LANES
    per_chunk = tokens // seg_len
    n_chunks = seg_count // per_chunk
    pairs = LANES // head_dim
    even = par_ref[0] == 0
    half = lax.rem(pl.program_id(0), 2)
    row = lax.broadcasted_iota(jnp.int32, (tokens, tokens), 0)
    col = lax.broadcasted_iota(jnp.int32, (tokens, tokens), 1)
    causal = row >= col
    first = col < head_dim

    left = lax.broadcasted_iota(jnp.int32, (16, tokens), 1) < seg_len
    dts = []
    for chunk in range(n_chunks):
        lo = dt_ref[per_chunk * chunk].astype(jnp.float32)
        hi = dt_ref[per_chunk * chunk + 1].astype(jnp.float32)
        lo = jnp.where(half == 0, lo, pltpu.roll(lo, seg_len, 1))
        hi = jnp.where(half == 0, pltpu.roll(hi, seg_len, 1), hi)
        dts.append(jnp.where(left, lo, hi))
    dt = jnp.concatenate(dts, axis=0)
    lane = lax.broadcasted_iota(jnp.int32, dt.shape, 1)
    cum = dt * jnp.concatenate([a_ref[...]] * n_chunks, axis=0)
    step = 1
    while step < tokens:
        cum = cum + jnp.where(lane >= step, pltpu.roll(cum, step, 1), 0.0)
        step *= 2
    last = cum[:, tokens - 1:]
    weight = jnp.exp(last - cum) * dt
    last_e = jnp.exp(last)
    cum_c = jnp.transpose(cum)

    state[...] = jnp.zeros_like(state)
    for chunk in range(n_chunks):
        segs = range(chunk * per_chunk, (chunk + 1) * per_chunk)
        tok = lambda ref, lo: jnp.concatenate([ref[s, lo:lo + seg_len] for s in segs], axis=0)
        mine = tok(mine_ref, 0)
        other = tok(other_ref, 0)
        b_mat = jnp.where(even, mine, other)
        c_mat = jnp.where(even, other, mine)
        scores = lax.dot_general(c_mat, b_mat, (((1,), (1,)), ((), ())), preferred_element_type=jnp.float32)
        if chunk:
            carried = lax.dot_general(c_mat, state[...].astype(jnp.bfloat16), (((1,), (1,)), ((), ())), preferred_element_type=jnp.float32)
        scaled = []
        for j in range(blocks):
            rows = [chunk * 16 + j * pairs + k for k in range(pairs)]
            mixes = []
            starts = []
            for h in rows:
                start = jnp.broadcast_to(cum_c[:, h:h + 1], (tokens, tokens))
                diff = jnp.where(causal, start - cum[h:h + 1, :], -jnp.inf)
                mixes.append((jnp.exp(diff) * (scores * dt[h:h + 1, :])).astype(jnp.bfloat16))
                starts.append(start)
            x2 = tok(x_ref, j * seg_len)
            zero = jnp.zeros_like(x2)
            stacked = jnp.concatenate([jnp.where(first, x2, zero), jnp.where(first, zero, x2)], axis=0)
            y = jnp.dot(jnp.concatenate(mixes, axis=1), stacked, preferred_element_type=jnp.float32)
            x_float = x2.astype(jnp.float32)
            y = y + d_ref[:, j * LANES:(j + 1) * LANES] * x_float
            if chunk:
                y = y + carried[:, j * LANES:(j + 1) * LANES] * jnp.exp(jnp.where(first, starts[0], starts[1]))
            y = y.astype(jnp.bfloat16)
            for k, s in enumerate(segs):
                y_ref[s, j * seg_len:(j + 1) * seg_len] = y[k * seg_len:(k + 1) * seg_len]
            x_t = jnp.transpose(x_float)
            for k, h in enumerate(rows):
                scaled.append((x_t[k * head_dim:(k + 1) * head_dim] * weight[h:h + 1, :]).astype(jnp.bfloat16))
        gain = jnp.dot(jnp.concatenate(scaled, axis=0), b_mat, preferred_element_type=jnp.float32)
        for h in range(n_local):
            part = slice(h * head_dim, (h + 1) * head_dim)
            new = gain[part]
            if chunk:
                new = new + state[part] * last_e[chunk * 16 + h:chunk * 16 + h + 1]
            if chunk == n_chunks - 1:
                fin_ref[0, 0, h] = new
            else:
                state[part] = new


def scan_call(parity, packed, other, a_neg, d_wide, finals, place, sizes):
    n_prompts, seg_len, seg_count, n_local, head_dim, d_state, batch, layers = sizes
    blocks = n_local * head_dim // LANES
    group = LANES // seg_len
    per_prompt = (blocks + 1) * seg_len
    dt_first = n_prompts * per_prompt // 16
    layer_index, first_prompt = place
    body = functools.partial(scan_kernel, seg_count, seg_len, blocks, n_local, head_dim)
    in_specs = [
        pl.BlockSpec(memory_space=pltpu.SMEM),
        pl.BlockSpec((seg_count, blocks * seg_len, LANES), lambda g: (0, g, 0)),
        pl.BlockSpec((seg_count, seg_len, LANES), lambda g: (0, n_prompts * blocks + g, 0)),
        pl.BlockSpec((seg_count, seg_len, LANES), lambda g: (0, g, 0)),
        pl.BlockSpec((seg_count, 16, LANES), lambda g: (0, dt_first + g // group, 0)),
        pl.BlockSpec((16, LANES), lambda g: (0, 0)),
        pl.BlockSpec((1, n_local * head_dim), lambda g: (0, 0)),
    ]
    operands = [parity, packed, packed, other, packed, a_neg, d_wide]
    aliases = {}
    if finals is not None:
        in_specs.append(pl.BlockSpec(memory_space=pl.ANY))
        operands.append(finals)
        aliases = {7: 1}
    tokens = n_prompts * seg_len * seg_count
    return pl.pallas_call(
        body,
        grid=(n_prompts,),
        in_specs=in_specs,
        out_specs=[
            pl.BlockSpec((seg_count, blocks * seg_len, LANES), lambda g: (0, g, 0)),
            pl.BlockSpec((1, 1, n_local, head_dim, d_state), lambda g: (first_prompt + g, layer_index, 0, 0, 0)),
        ],
        out_shape=[
            jax.ShapeDtypeStruct((seg_count, n_prompts * blocks * seg_len, LANES), jnp.bfloat16),
            jax.ShapeDtypeStruct((batch, layers, n_local, head_dim, d_state), jnp.float32),
        ],
        scratch_shapes=[pltpu.VMEM((n_local * head_dim, d_state), jnp.float32)],
        input_output_aliases=aliases,
        cost_estimate=pl.CostEstimate(flops=tokens * n_local * 16000, bytes_accessed=tokens * n_local * head_dim * 6, transcendentals=tokens * n_local * LANES),
        name='scan',
    )(*operands)


def gate_kernel(n_src, blocks, seg_len, y_ref, z_ref, w_ref, out_ref, keep):
    total = jnp.zeros((seg_len, LANES), jnp.float32)
    for d in range(n_src):
        for j in range(blocks):
            cols = slice((d * blocks + j) * LANES, (d * blocks + j + 1) * LANES)
            z = z_ref[:, cols].astype(jnp.float32)
            g = y_ref[d, j * seg_len:(j + 1) * seg_len].astype(jnp.float32) * (z * jax.nn.sigmoid(z))
            keep[:, cols] = g
            total = total + g * g
    width = n_src * blocks * LANES
    scale = lax.rsqrt(jnp.sum(total, axis=1, keepdims=True) / width + EPSILON)
    for i in range(n_src * blocks):
        cols = slice(i * LANES, (i + 1) * LANES)
        out_ref[:, cols] = (keep[:, cols] * scale * w_ref[:, cols]).astype(jnp.bfloat16)


def gate_call(y, u, gate_w, n_prompts, seg_len, d_inner):
    n_src = y.shape[0]
    blocks = d_inner // n_src // LANES
    tokens = n_prompts * seg_len
    return pl.pallas_call(
        functools.partial(gate_kernel, n_src, blocks, seg_len),
        grid=(n_prompts,),
        in_specs=[
            pl.BlockSpec((n_src, blocks * seg_len, LANES), lambda p: (0, p, 0)),
            pl.BlockSpec((seg_len, d_inner), lambda p: (p, 0)),
            pl.BlockSpec((1, d_inner), lambda p: (0, 0)),
        ],
        out_specs=pl.BlockSpec((seg_len, d_inner), lambda p: (p, 0)),
        out_shape=jax.ShapeDtypeStruct((tokens, d_inner), jnp.bfloat16),
        scratch_shapes=[pltpu.VMEM((seg_len, d_inner), jnp.float32)],
        cost_estimate=pl.CostEstimate(flops=tokens * d_inner * 40, bytes_accessed=6 * tokens * d_inner, transcendentals=tokens * d_inner),
        name='gate',
    )(y, u, gate_w)


def solution(mesh):
    seg_count = mesh.shape['sp']

    def forward(resid, pre_norm, w_in, conv_w, conv_b, dt_bias, a_log, d_skip, gate_norm, w_out):
        batch, seg_len, d_model = resid.shape
        layers, n_heads = dt_bias.shape
        conv_dim = conv_b.shape[1]
        d_inner = gate_norm.shape[1] * gate_norm.shape[2]
        d_state = (conv_dim - d_inner) // 2
        head_dim = d_inner // n_heads
        n_local = n_heads // seg_count
        blocks = n_local * head_dim // LANES
        taps = CONV_WIDTH - 1
        seg_index = lax.axis_index('sp')
        parity = lax.rem(seg_index, 2).astype(jnp.int32).reshape(1)
        forward_pairs = [(source, source + 1) for source in range(seg_count - 1)]
        core_pairs = [(source, source ^ 1) for source in range(seg_count)]

        slot = jnp.arange(seg_count * 16)
        wanted = jnp.where(slot % 16 < n_local, slot // 16 * n_local + slot % 16, -1)
        select = (wanted[:, None] == jnp.arange(LANES)[None, :]).astype(jnp.bfloat16)
        pad_heads = lambda values: jnp.pad(values, ((0, 0), (0, LANES - n_heads)))
        dt_bias_wide = pad_heads(dt_bias)
        conv_wt = jnp.swapaxes(conv_w, 1, 2)

        finals = None
        starts = [sum(SIZES[:c]) for c in range(len(SIZES))]
        streams = [resid[starts[c]:starts[c] + SIZES[c]].reshape(SIZES[c] * seg_len, d_model) for c in range(len(SIZES))]
        tails = [[] for _ in range(layers)]
        last_seg = seg_count - 1
        hops = [[(last_seg, 1)], [(last_seg, last_seg - 2), (1, 3)], [(source, source - 1) for source in range(1, seg_count, 2)]]

        def spread(rows, hop):
            got = lax.ppermute(rows, 'sp', hop)
            takes = functools.reduce(jnp.logical_or, [seg_index == dest for _, dest in hop])
            return jnp.where(takes, got, rows)

        for l in range(layers):
            final_layer = l == layers - 1
            mine = lax.dynamic_slice_in_dim(a_log[l], seg_index * n_local, n_local)
            a_neg = jnp.broadcast_to(jnp.pad(-jnp.exp(mine), (0, 16 - n_local))[:, None], (16, LANES))
            d_wide = jnp.repeat(lax.dynamic_slice_in_dim(d_skip[l], seg_index * n_local, n_local), head_dim)[None]
            packs, gates = [], []
            for c, n_prompts in enumerate(SIZES):
                if c > 0:
                    streams[c], tails[l][c - 1] = lax.optimization_barrier((streams[c], tails[l][c - 1]))
                r = streams[c]
                h = (r * lax.rsqrt(jnp.mean(r * r, axis=-1, keepdims=True) + EPSILON) * pre_norm[l]).astype(jnp.bfloat16)
                u = jnp.dot(h, w_in[l, :, d_inner:], preferred_element_type=jnp.float32).astype(jnp.bfloat16)
                tail = tail_call(u, n_prompts, seg_len, conv_dim)
                tails[l].append(tail)
                halo = lax.ppermute(tail, 'sp', forward_pairs)
                packed = conv_call(u, halo, conv_wt[l], conv_b[l:l + 1], dt_bias_wide[l:l + 1], select, (n_prompts, seg_len, d_inner, conv_dim, n_heads, seg_count))
                packed, h = lax.optimization_barrier((packed, h))
                packs.append(packed)
                gates.append(jnp.dot(h, w_in[l, :, :d_inner], preferred_element_type=jnp.float32).astype(jnp.bfloat16))
            if final_layer:
                tail_rows = jnp.concatenate([rows for layer_rows in tails for rows in layer_rows], axis=1)
            outs, arrived = [], []
            for c in range(len(SIZES)):
                arrived.append(lax.all_to_all(packs[c], 'sp', 0, 0, tiled=True))
            if final_layer:
                arrived[-1], tail_rows = lax.optimization_barrier((arrived[-1], spread(tail_rows, hops[0])))
            for c, n_prompts in enumerate(SIZES):
                packed = arrived[c]
                bc_start = n_prompts * blocks * seg_len
                bc = packed[:, bc_start:bc_start + n_prompts * seg_len]
                other = lax.ppermute(bc, 'sp', core_pairs)
                y, finals = scan_call(parity, packed, other, a_neg, d_wide, finals, (l, starts[c]), (n_prompts, seg_len, seg_count, n_local, head_dim, d_state, batch, layers))
                y = lax.all_to_all(y, 'sp', 0, 0, tiled=True)
                if final_layer and c >= len(SIZES) - 2:
                    y, tail_rows = lax.optimization_barrier((y, spread(tail_rows, hops[c - len(SIZES) + 3])))
                outs.append(y)
            for c, n_prompts in enumerate(SIZES):
                g = gate_call(outs[c], gates[c], gate_norm[l], n_prompts, seg_len, d_inner)
                streams[c] = streams[c] + jnp.dot(g, w_out[l], preferred_element_type=jnp.float32)
        out = jnp.concatenate(streams, axis=0).reshape(batch, seg_len, d_model)
        conv_state = tail_rows.reshape(taps, layers, batch, conv_dim)
        return out, finals, jnp.transpose(conv_state, (2, 1, 3, 0))

    return jax.shard_map(forward, mesh=mesh, in_specs=(P('dp', 'sp', None), P(), P(), P(), P(), P(), P(), P(), P(), P()), out_specs=(P('dp', 'sp', None), P('dp', None, 'sp', None, None), P('dp', None, None, None)), check_vma=False)
```

```python
import functools

import jax
import jax.numpy as jnp
from jax import lax
from jax.experimental import pallas as pl
from jax.experimental.pallas import tpu as pltpu
from jax.sharding import PartitionSpec as P


CONV_WIDTH = 4
EPSILON = 1e-5
LANES = 128
SIZES = (8, 8)


def silu(values):
    half = 0.5 * values
    return half + half * jnp.tanh(half)


def conv_kernel(n_prompts, seg_len, width, n_heads, x_ref, bc_ref, dtr_ref, xh_ref, bch_ref, wx_ref, wbc_ref, bx_ref, bbc_ref, dtb_ref, sel_ref, out_ref, bc_keep, dt_keep):
    dest = pl.program_id(0)
    taps = CONV_WIDTH - 1
    blocks = width // LANES

    def conv(cur, halo, w, bias):
        cur = cur.astype(jnp.float32)
        halo = halo.astype(jnp.float32)
        acc = bias + cur * w[taps:taps + 1]
        for back in range(1, CONV_WIDTH):
            shifted = jnp.concatenate([halo[taps - back:], cur[:seg_len - back]], axis=0)
            acc = acc + shifted * w[taps - back:taps - back + 1]
        return silu(acc).astype(jnp.bfloat16)

    @pl.when(dest == 0)
    def _():
        raw = dtr_ref[...].astype(jnp.float32)
        column = lax.broadcasted_iota(jnp.int32, raw.shape, 1)
        delta = jax.nn.softplus(raw + dtb_ref[...])
        delta = jnp.where(column < n_heads, delta, 0.0).astype(jnp.bfloat16)
        rows = lax.dot_general(sel_ref[...], delta, (((1,), (1,)), ((), ())), preferred_element_type=jnp.float32)
        rows = rows.astype(jnp.bfloat16)
        for d in range(dt_keep.shape[0]):
            for part in range(dt_keep.shape[1] // 16):
                dt_keep[d, part * 16:(part + 1) * 16] = rows[d * 16:(d + 1) * 16, part * LANES:(part + 1) * LANES]

    @pl.when(dest < 2)
    def _():
        for p in range(n_prompts):
            bc_keep[dest, p] = conv(bc_ref[p * seg_len:(p + 1) * seg_len], bch_ref[:, p], wbc_ref[...], bbc_ref[...])

    parity = lax.rem(dest, 2)
    per_prompt = blocks * seg_len
    bc_start = n_prompts * per_prompt
    for p in range(n_prompts):
        for j in range(blocks):
            cols = slice(j * LANES, (j + 1) * LANES)
            out_ref[0, p * per_prompt + j * seg_len:p * per_prompt + (j + 1) * seg_len] = conv(
                x_ref[p * seg_len:(p + 1) * seg_len, cols], xh_ref[:, p, cols], wx_ref[:, cols], bx_ref[:, cols])
        out_ref[0, bc_start + p * seg_len:bc_start + (p + 1) * seg_len] = bc_keep[parity, p]
    out_ref[0, bc_start + n_prompts * seg_len:] = dt_keep[dest]


def tail_kernel(*refs):
    taps = CONV_WIDTH - 1
    out_ref = refs[-1]
    rows = [ref[...].astype(jnp.float32)[16 - taps:] for ref in refs[:-1]]
    for k in range(taps):
        out_ref[k] = jnp.concatenate([row[k:k + 1] for row in rows], axis=0).astype(jnp.bfloat16)


def tail_call(u, n_prompts, seg_len, conv_dim):
    taps = CONV_WIDTH - 1
    width = conv_dim // 2
    step = seg_len // 16
    return pl.pallas_call(
        tail_kernel,
        grid=(2,),
        in_specs=[pl.BlockSpec((16, width), lambda i, p=p: ((p + 1) * step - 1, i)) for p in range(n_prompts)],
        out_specs=pl.BlockSpec((taps, n_prompts, width), lambda i: (0, 0, i)),
        out_shape=jax.ShapeDtypeStruct((taps, n_prompts, conv_dim), jnp.bfloat16),
        cost_estimate=pl.CostEstimate(flops=n_prompts * conv_dim * 100, bytes_accessed=40 * n_prompts * conv_dim, transcendentals=0),
        name='tail',
    )(*[u] * n_prompts)


def conv_call(u, halo, conv_w, conv_b, dt_b, select, sizes):
    n_prompts, seg_len, d_inner, conv_dim, n_heads, n_dest = sizes
    width = d_inner // n_dest
    blocks = width // LANES
    dt_rows = n_prompts * seg_len // LANES * 16
    rows = n_prompts * (blocks + 1) * seg_len + dt_rows
    tokens = n_prompts * seg_len
    bc0 = d_inner // LANES
    dt0 = conv_dim // LANES
    taps = CONV_WIDTH - 1
    body = functools.partial(conv_kernel, n_prompts, seg_len, width, n_heads)
    parity = lambda d: lax.rem(d, 2)
    return pl.pallas_call(
        body,
        grid=(n_dest,),
        in_specs=[
            pl.BlockSpec((tokens, width), lambda d: (0, d)),
            pl.BlockSpec((tokens, LANES), lambda d: (0, bc0 + parity(d))),
            pl.BlockSpec((tokens, LANES), lambda d: (0, dt0)),
            pl.BlockSpec((taps, n_prompts, width), lambda d: (0, 0, d)),
            pl.BlockSpec((taps, n_prompts, LANES), lambda d: (0, 0, d_inner // LANES + parity(d))),
            pl.BlockSpec((CONV_WIDTH, width), lambda d: (0, d)),
            pl.BlockSpec((CONV_WIDTH, LANES), lambda d: (0, d_inner // LANES + parity(d))),
            pl.BlockSpec((1, width), lambda d: (0, d)),
            pl.BlockSpec((1, LANES), lambda d: (0, d_inner // LANES + parity(d))),
            pl.BlockSpec((1, LANES), lambda d: (0, 0)),
            pl.BlockSpec((n_dest * 16, LANES), lambda d: (0, 0)),
        ],
        out_specs=pl.BlockSpec((1, rows, LANES), lambda d: (d, 0, 0)),
        out_shape=jax.ShapeDtypeStruct((n_dest, rows, LANES), jnp.bfloat16),
        scratch_shapes=[
            pltpu.VMEM((2, n_prompts, seg_len, LANES), jnp.bfloat16),
            pltpu.VMEM((n_dest, dt_rows, LANES), jnp.bfloat16),
        ],
        cost_estimate=pl.CostEstimate(flops=tokens * d_inner * 60, bytes_accessed=4 * tokens * d_inner, transcendentals=tokens * d_inner),
        name='conv_pack',
    )(u, u, u, halo, halo, conv_w, conv_w, conv_b, conv_b, dt_b, select)


def scan_kernel(seg_count, seg_len, blocks, n_local, head_dim, par_ref, x_ref, mine_ref, other_ref, dt_ref, a_ref, d_ref, *rest):
    y_ref, fin_ref, state = rest[-3:]
    tokens = LANES
    per_chunk = tokens // seg_len
    n_chunks = seg_count // per_chunk
    pairs = LANES // head_dim
    even = par_ref[0] == 0
    half = lax.rem(pl.program_id(0), 2)
    row = lax.broadcasted_iota(jnp.int32, (tokens, tokens), 0)
    col = lax.broadcasted_iota(jnp.int32, (tokens, tokens), 1)
    causal = row >= col
    first = col < head_dim

    left = lax.broadcasted_iota(jnp.int32, (16, tokens), 1) < seg_len
    dts = []
    for chunk in range(n_chunks):
        lo = dt_ref[per_chunk * chunk].astype(jnp.float32)
        hi = dt_ref[per_chunk * chunk + 1].astype(jnp.float32)
        lo = jnp.where(half == 0, lo, pltpu.roll(lo, seg_len, 1))
        hi = jnp.where(half == 0, pltpu.roll(hi, seg_len, 1), hi)
        dts.append(jnp.where(left, lo, hi))
    dt = jnp.concatenate(dts, axis=0)
    lane = lax.broadcasted_iota(jnp.int32, dt.shape, 1)
    cum = dt * jnp.concatenate([a_ref[...]] * n_chunks, axis=0)
    step = 1
    while step < tokens:
        cum = cum + jnp.where(lane >= step, pltpu.roll(cum, step, 1), 0.0)
        step *= 2
    last = cum[:, tokens - 1:]
    weight = jnp.exp(last - cum) * dt
    last_e = jnp.exp(last)
    cum_c = jnp.transpose(cum)

    state[...] = jnp.zeros_like(state)
    for chunk in range(n_chunks):
        segs = range(chunk * per_chunk, (chunk + 1) * per_chunk)
        tok = lambda ref, lo: jnp.concatenate([ref[s, lo:lo + seg_len] for s in segs], axis=0)
        mine = tok(mine_ref, 0)
        other = tok(other_ref, 0)
        b_mat = jnp.where(even, mine, other)
        c_mat = jnp.where(even, other, mine)
        scores = lax.dot_general(c_mat, b_mat, (((1,), (1,)), ((), ())), preferred_element_type=jnp.float32)
        if chunk:
            carried = lax.dot_general(c_mat, state[...].astype(jnp.bfloat16), (((1,), (1,)), ((), ())), preferred_element_type=jnp.float32)
        scaled = []
        for j in range(blocks):
            rows = [chunk * 16 + j * pairs + k for k in range(pairs)]
            mixes = []
            starts = []
            for h in rows:
                start = jnp.broadcast_to(cum_c[:, h:h + 1], (tokens, tokens))
                diff = jnp.where(causal, start - cum[h:h + 1, :], -jnp.inf)
                mixes.append((jnp.exp(diff) * (scores * dt[h:h + 1, :])).astype(jnp.bfloat16))
                starts.append(start)
            x2 = tok(x_ref, j * seg_len)
            zero = jnp.zeros_like(x2)
            stacked = jnp.concatenate([jnp.where(first, x2, zero), jnp.where(first, zero, x2)], axis=0)
            y = jnp.dot(jnp.concatenate(mixes, axis=1), stacked, preferred_element_type=jnp.float32)
            x_float = x2.astype(jnp.float32)
            y = y + d_ref[:, j * LANES:(j + 1) * LANES] * x_float
            if chunk:
                y = y + carried[:, j * LANES:(j + 1) * LANES] * jnp.exp(jnp.where(first, starts[0], starts[1]))
            y = y.astype(jnp.bfloat16)
            for k, s in enumerate(segs):
                y_ref[s, j * seg_len:(j + 1) * seg_len] = y[k * seg_len:(k + 1) * seg_len]
            x_t = jnp.transpose(x_float)
            for k, h in enumerate(rows):
                scaled.append((x_t[k * head_dim:(k + 1) * head_dim] * weight[h:h + 1, :]).astype(jnp.bfloat16))
        gain = jnp.dot(jnp.concatenate(scaled, axis=0), b_mat, preferred_element_type=jnp.float32)
        for h in range(n_local):
            part = slice(h * head_dim, (h + 1) * head_dim)
            new = gain[part]
            if chunk:
                new = new + state[part] * last_e[chunk * 16 + h:chunk * 16 + h + 1]
            if chunk == n_chunks - 1:
                fin_ref[0, 0, h] = new
            else:
                state[part] = new


def scan_call(parity, packed, other, a_neg, d_wide, finals, place, sizes):
    n_prompts, seg_len, seg_count, n_local, head_dim, d_state, batch, layers = sizes
    blocks = n_local * head_dim // LANES
    group = LANES // seg_len
    per_prompt = (blocks + 1) * seg_len
    dt_first = n_prompts * per_prompt // 16
    layer_index, first_prompt = place
    body = functools.partial(scan_kernel, seg_count, seg_len, blocks, n_local, head_dim)
    in_specs = [
        pl.BlockSpec(memory_space=pltpu.SMEM),
        pl.BlockSpec((seg_count, blocks * seg_len, LANES), lambda g: (0, g, 0)),
        pl.BlockSpec((seg_count, seg_len, LANES), lambda g: (0, n_prompts * blocks + g, 0)),
        pl.BlockSpec((seg_count, seg_len, LANES), lambda g: (0, g, 0)),
        pl.BlockSpec((seg_count, 16, LANES), lambda g: (0, dt_first + g // group, 0)),
        pl.BlockSpec((16, LANES), lambda g: (0, 0)),
        pl.BlockSpec((1, n_local * head_dim), lambda g: (0, 0)),
    ]
    operands = [parity, packed, packed, other, packed, a_neg, d_wide]
    aliases = {}
    if finals is not None:
        in_specs.append(pl.BlockSpec(memory_space=pl.ANY))
        operands.append(finals)
        aliases = {7: 1}
    tokens = n_prompts * seg_len * seg_count
    return pl.pallas_call(
        body,
        grid=(n_prompts,),
        in_specs=in_specs,
        out_specs=[
            pl.BlockSpec((seg_count, blocks * seg_len, LANES), lambda g: (0, g, 0)),
            pl.BlockSpec((1, 1, n_local, head_dim, d_state), lambda g: (first_prompt + g, layer_index, 0, 0, 0)),
        ],
        out_shape=[
            jax.ShapeDtypeStruct((seg_count, n_prompts * blocks * seg_len, LANES), jnp.bfloat16),
            jax.ShapeDtypeStruct((batch, layers, n_local, head_dim, d_state), jnp.float32),
        ],
        scratch_shapes=[pltpu.VMEM((n_local * head_dim, d_state), jnp.float32)],
        input_output_aliases=aliases,
        cost_estimate=pl.CostEstimate(flops=tokens * n_local * 16000, bytes_accessed=tokens * n_local * head_dim * 6, transcendentals=tokens * n_local * LANES),
        name='scan',
    )(*operands)


def gate_kernel(n_src, blocks, seg_len, group, y_ref, z_ref, w_ref, out_ref, keep):
    width = n_src * blocks * LANES
    for p in range(group):
        rows = slice(p * seg_len, (p + 1) * seg_len)
        total = jnp.zeros((seg_len, LANES), jnp.float32)
        for d in range(n_src):
            for j in range(blocks):
                cols = slice((d * blocks + j) * LANES, (d * blocks + j + 1) * LANES)
                z = z_ref[rows, cols].astype(jnp.float32)
                y = y_ref[d, (p * blocks + j) * seg_len:(p * blocks + j + 1) * seg_len].astype(jnp.float32)
                g = y * silu(z)
                keep[p, :, cols] = g
                total = total + g * g
        scale = lax.rsqrt(jnp.sum(total, axis=1, keepdims=True) / width + EPSILON)
        for i in range(n_src * blocks):
            cols = slice(i * LANES, (i + 1) * LANES)
            out_ref[rows, cols] = (keep[p, :, cols] * scale * w_ref[:, cols]).astype(jnp.bfloat16)


def gate_call(y, u, gate_w, n_prompts, seg_len, d_inner):
    n_src = y.shape[0]
    blocks = d_inner // n_src // LANES
    tokens = n_prompts * seg_len
    group = 2
    return pl.pallas_call(
        functools.partial(gate_kernel, n_src, blocks, seg_len, group),
        grid=(n_prompts // group,),
        in_specs=[
            pl.BlockSpec((n_src, group * blocks * seg_len, LANES), lambda p: (0, p, 0)),
            pl.BlockSpec((group * seg_len, d_inner), lambda p: (p, 0)),
            pl.BlockSpec((1, d_inner), lambda p: (0, 0)),
        ],
        out_specs=pl.BlockSpec((group * seg_len, d_inner), lambda p: (p, 0)),
        out_shape=jax.ShapeDtypeStruct((tokens, d_inner), jnp.bfloat16),
        scratch_shapes=[pltpu.VMEM((group, seg_len, d_inner), jnp.float32)],
        cost_estimate=pl.CostEstimate(flops=tokens * d_inner * 40, bytes_accessed=6 * tokens * d_inner, transcendentals=tokens * d_inner),
        name='gate',
    )(y, u, gate_w)


def solution(mesh):
    seg_count = mesh.shape['sp']

    def forward(resid, pre_norm, w_in, conv_w, conv_b, dt_bias, a_log, d_skip, gate_norm, w_out):
        batch, seg_len, d_model = resid.shape
        layers, n_heads = dt_bias.shape
        conv_dim = conv_b.shape[1]
        d_inner = gate_norm.shape[1] * gate_norm.shape[2]
        d_state = (conv_dim - d_inner) // 2
        head_dim = d_inner // n_heads
        n_local = n_heads // seg_count
        blocks = n_local * head_dim // LANES
        taps = CONV_WIDTH - 1
        seg_index = lax.axis_index('sp')
        parity = lax.rem(seg_index, 2).astype(jnp.int32).reshape(1)
        forward_pairs = [(source, source + 1) for source in range(seg_count - 1)]
        core_pairs = [(source, source ^ 1) for source in range(seg_count)]

        slot = jnp.arange(seg_count * 16)
        wanted = jnp.where(slot % 16 < n_local, slot // 16 * n_local + slot % 16, -1)
        select = (wanted[:, None] == jnp.arange(LANES)[None, :]).astype(jnp.bfloat16)
        pad_heads = lambda values: jnp.pad(values, ((0, 0), (0, LANES - n_heads)))
        dt_bias_wide = pad_heads(dt_bias)
        conv_wt = jnp.swapaxes(conv_w, 1, 2)

        finals = None
        starts = [sum(SIZES[:c]) for c in range(len(SIZES))]
        streams = [resid[starts[c]:starts[c] + SIZES[c]].reshape(SIZES[c] * seg_len, d_model) for c in range(len(SIZES))]
        tails = []
        resid_halo = lax.ppermute(jnp.swapaxes(resid[:, seg_len - taps:], 0, 1), 'sp', forward_pairs)
        last_seg = seg_count - 1
        hops = [[(last_seg, 1)], [(last_seg, last_seg - 2), (1, 3)], [(source, source - 1) for source in range(1, seg_count, 2)]]

        def spread(rows, hop):
            got = lax.ppermute(rows, 'sp', hop)
            takes = functools.reduce(jnp.logical_or, [seg_index == dest for _, dest in hop])
            return jnp.where(takes, got, rows)

        for l in range(layers):
            final_layer = l == layers - 1
            mine = lax.dynamic_slice_in_dim(a_log[l], seg_index * n_local, n_local)
            a_neg = jnp.broadcast_to(jnp.pad(-jnp.exp(mine), (0, 16 - n_local))[:, None], (16, LANES))
            d_wide = jnp.repeat(lax.dynamic_slice_in_dim(d_skip[l], seg_index * n_local, n_local), head_dim)[None]
            packs, gates = [], []
            for c, n_prompts in enumerate(SIZES):
                r = streams[c]
                tokens = n_prompts * seg_len
                mean_sq = jnp.mean(r * r, axis=-1, keepdims=True)
                if tails:
                    mean_sq, tails[-1] = lax.optimization_barrier((mean_sq, tails[-1]))
                h = (r * lax.rsqrt(mean_sq + EPSILON) * pre_norm[l]).astype(jnp.bfloat16)
                rows = h
                if l == 0:
                    early = resid_halo[:, starts[c]:starts[c] + n_prompts].reshape(taps * n_prompts, d_model)
                    early = early * lax.rsqrt(jnp.mean(early * early, axis=-1, keepdims=True) + EPSILON) * pre_norm[l]
                    rows = jnp.concatenate([h, early.astype(jnp.bfloat16)], axis=0)
                u = jnp.dot(rows, w_in[l, :, d_inner:], preferred_element_type=jnp.float32).astype(jnp.bfloat16)
                tail = tail_call(u, n_prompts, seg_len, conv_dim)
                tails.append(tail)
                if l == 0:
                    halo = u[tokens:, :conv_dim].reshape(taps, n_prompts, conv_dim)
                else:
                    halo = lax.ppermute(tail, 'sp', forward_pairs)
                packed = conv_call(u, halo, conv_wt[l], conv_b[l:l + 1], dt_bias_wide[l:l + 1], select, (n_prompts, seg_len, d_inner, conv_dim, n_heads, seg_count))
                packed, h = lax.optimization_barrier((packed, h))
                packs.append(packed)
                gates.append(jnp.dot(h, w_in[l, :, :d_inner], preferred_element_type=jnp.float32).astype(jnp.bfloat16))
            if final_layer:
                tail_rows = jnp.concatenate(tails, axis=1)
            outs, arrived = [], []
            for c in range(len(SIZES)):
                arrived.append(lax.all_to_all(packs[c], 'sp', 0, 0, tiled=True))
            if final_layer:
                arrived[-1], tail_rows = lax.optimization_barrier((arrived[-1], spread(tail_rows, hops[0])))
            for c, n_prompts in enumerate(SIZES):
                packed = arrived[c]
                bc_start = n_prompts * blocks * seg_len
                bc = packed[:, bc_start:bc_start + n_prompts * seg_len]
                other = lax.ppermute(bc, 'sp', core_pairs)
                y, finals = scan_call(parity, packed, other, a_neg, d_wide, finals, (l, starts[c]), (n_prompts, seg_len, seg_count, n_local, head_dim, d_state, batch, layers))
                y = lax.all_to_all(y, 'sp', 0, 0, tiled=True)
                if final_layer and c >= len(SIZES) - 2:
                    if c == len(SIZES) - 1:
                        tail_rows = spread(tail_rows, hops[1])
                    y, tail_rows = lax.optimization_barrier((y, tail_rows))
                outs.append(y)
            for c, n_prompts in enumerate(SIZES):
                g = gate_call(outs[c], gates[c], gate_norm[l], n_prompts, seg_len, d_inner)
                streams[c] = streams[c] + jnp.dot(g, w_out[l], preferred_element_type=jnp.float32)
        out = jnp.zeros((batch * seg_len, d_model), jnp.float32)
        for c in range(len(SIZES)):
            out = lax.optimization_barrier(lax.dynamic_update_slice(out, streams[c], (starts[c] * seg_len, 0)))
        out = out.reshape(batch, seg_len, d_model)
        conv_state = spread(tail_rows, hops[2]).reshape(taps, layers, batch, conv_dim)
        return out, finals, jnp.transpose(conv_state, (2, 1, 3, 0))

    return jax.shard_map(forward, mesh=mesh, in_specs=(P('dp', 'sp', None), P(), P(), P(), P(), P(), P(), P(), P(), P()), out_specs=(P('dp', 'sp', None), P('dp', None, 'sp', None, None), P('dp', None, None, None)), check_vma=False)
```
